32 devices in a mesh: rep: 1, dp: 32 (over x, y, z, core).
Axes of the slice: x: 2, y: 2, z: 4, core: 2. Of those that a mesh axis runs over, the one named last changes fastest.
Arguments:
- x: bfloat16 [32, 2048, 1024], P(('rep', 'dp'))
- dy: bfloat16 [32, 2048, 1024], P(('rep', 'dp'))
- w_gate: bfloat16 [2, 1024, 2560], replicated
- w_up: bfloat16 [2, 1024, 2560], replicated
- w_down: bfloat16 [2, 2560, 1024], replicated
- m_w_gate: float32 [2, 1024, 2560], replicated
- m_w_up: float32 [2, 1024, 2560], replicated
- m_w_down: float32 [2, 2560, 1024], replicated
- v_w_gate: float32 [2, 1024, 2560], replicated
- v_w_up: float32 [2, 1024, 2560], replicated
- v_w_down: float32 [2, 2560, 1024], replicated
Outputs:
- output 1: bfloat16 [2, 1024, 2560], P('rep')
- output 2: bfloat16 [2, 1024, 2560], P('rep')
- output 3: bfloat16 [2, 2560, 1024], P('rep')
- output 4: float32 [2, 1024, 2560], P('rep')
- output 5: float32 [2, 1024, 2560], P('rep')
- output 6: float32 [2, 2560, 1024], P('rep')
- output 7: float32 [2, 1024, 2560], P('rep')
- output 8: float32 [2, 1024, 2560], P('rep')
- output 9: float32 [2, 2560, 1024], P('rep')
All inputs are finite; a program needn't handle non-finite values.
Results may differ from the reference program's by a relative error of at most 0.022.
Values are sent between devices in bfloat16 or wider.
A program may use at most 2.5 GiB of HBM per device.

```python
import jax
import jax.numpy as jnp
from jax import lax

SEQUENCES = 32
TOKENS = 2048
D = 1024
FF = 2560
LAYERS = 2
NAMES = ("w_gate", "w_up", "w_down")
SHAPES = {"w_gate": (LAYERS, D, FF), "w_up": (LAYERS, D, FF), "w_down": (LAYERS, FF, D)}


def bump(key, n, height):
    away = (jnp.arange(n, dtype=jnp.int32) - jax.random.randint(key, (), 0, n, jnp.int32)) % n
    return jnp.where(away < n // 8, height, 1.0)


def together(key, own, strength):
    shared = jax.random.normal(key, own.shape[1:], jnp.float32)
    return (own + strength * shared) * lax.rsqrt(1 + strength * strength)


def setup_inputs(seed: int = 0, part: int = 0) -> dict:
    kx, kdy, ka, kb, kz, kf, kh, kl, *keys = jax.random.split(jax.random.key(seed), 8 + 3 * len(NAMES))
    kx, kdy, ka, kb = (jax.random.fold_in(k, part) for k in (kx, kdy, ka, kb))
    kw, km, kv = (keys[i::3] for i in range(3))
    shape = (SEQUENCES, TOKENS, D)
    much_x, much_dy = jax.random.uniform(kz, (2,), jnp.float32, 0.0, 1.0)
    loud = 2.0 ** jax.random.uniform(jax.random.fold_in(kz, 1), (), jnp.float32, -1.0, 2.0)
    layers = 2.0 ** jax.random.uniform(kl, (LAYERS, 1, 1), jnp.float32, -1.0, 1.0)
    x = together(ka, jax.random.normal(kx, shape, jnp.float32), much_x) * bump(kf, D, 4.0)
    dy = together(kb, jax.random.normal(kdy, shape, jnp.float32), much_dy)
    drawn = {"x": x.astype(jnp.bfloat16), "dy": (loud * dy * (SEQUENCES * TOKENS) ** -0.5).astype(jnp.bfloat16)}
    for key, name in zip(kw, NAMES, strict=True):
        w = jax.random.normal(key, SHAPES[name], jnp.float32) * SHAPES[name][1] ** -0.5
        drawn[name] = (w * {"w_gate": 1.0, "w_up": bump(kh, FF, 4.0), "w_down": layers}[name]).astype(jnp.bfloat16)
    for key, name in zip(km, NAMES, strict=True):
        drawn[f"m_{name}"] = 0.1 * jax.random.normal(key, SHAPES[name], jnp.float32)
    for key, name in zip(kv, NAMES, strict=True):
        drawn[f"v_{name}"] = jax.random.uniform(key, SHAPES[name], jnp.float32, 0.005, 0.015)
    return drawn


def matmul(a, w):
    return jnp.dot(a, w, preferred_element_type=jnp.float32).astype(jnp.bfloat16)


def normed(h):
    wide = h.astype(jnp.float32)
    scale = lax.rsqrt(jnp.mean(wide**2, -1, keepdims=True) + 1e-6)
    return (wide * scale).astype(jnp.bfloat16)


def layer(h, w):
    a = normed(h)
    gate = jnp.dot(a, w["w_gate"], preferred_element_type=jnp.float32)
    up = jnp.dot(a, w["w_up"], preferred_element_type=jnp.float32)
    return h + matmul((jax.nn.silu(gate) * up).astype(jnp.bfloat16), w["w_down"])


def adamw(w, m, v, g):
    m = 0.9 * m + 0.1 * g
    v = 0.95 * v + 0.05 * g * g
    step = m * lax.rsqrt(v + 1e-8) + 0.1 * w
    return (w - 0.02 * step).astype(jnp.bfloat16), m, v


def clipped(gradients, sum_of_squares, count):
    factor = jnp.minimum(1.0, 0.5 * lax.rsqrt(sum_of_squares / count + 1e-30))
    return [g * factor for g in gradients]


def stack(weights, h):
    return lax.scan(lambda h, w: (layer(h, w), None), h, weights)[0]


def reference(x, dy, w_gate, w_up, w_down, m_w_gate, m_w_up, m_w_down, v_w_gate, v_w_up, v_w_down):
    weights = dict(zip(NAMES, (w_gate, w_up, w_down), strict=True))

    def take(so_far, sequence):
        h, by_y = sequence
        _, back = jax.vjp(lambda w: stack(w, h), weights)
        return jax.tree.map(lambda total, term: total + term.astype(jnp.float32), so_far, back(by_y)[0]), None

    none_yet = {name: jnp.zeros(w.shape, jnp.float32) for name, w in weights.items()}
    by_weights, _ = lax.scan(take, none_yet, (x, dy))
    gradients = [by_weights[name].astype(jnp.bfloat16).astype(jnp.float32) for name in NAMES]
    gradients = clipped(gradients, sum(jnp.sum(g * g) for g in gradients), sum(g.size for g in gradients))
    new = [
        adamw(w.astype(jnp.float32), m, v, g)
        for w, m, v, g in zip((w_gate, w_up, w_down), (m_w_gate, m_w_up, m_w_down), (v_w_gate, v_w_up, v_w_down), gradients, strict=True)
    ]
    return tuple(one[which] for which in range(3) for one in new)
```

```python
import functools

import jax
import jax.numpy as jnp
from jax import lax
from jax.experimental import pallas as pl
from jax.experimental.pallas import tpu as pltpu
from jax.sharding import PartitionSpec as P

NAMES = ("w_gate", "w_up", "w_down")
MESH = pl.DeviceIdType.MESH
LIMIT = 66_000_000
CORE, Z1, Z2, Y, X = 1, 2, 4, 8, 16
ORDERS = ((X, Z1, Y, Z2), (Y, Z1, X, Z2))


def matmul(a, w):
    return jnp.dot(a, w, preferred_element_type=jnp.float32).astype(jnp.bfloat16)


def normed(h):
    wide = h.astype(jnp.float32)
    scale = lax.rsqrt(jnp.mean(wide**2, -1, keepdims=True) + 1e-6)
    return (wide * scale).astype(jnp.bfloat16)


def layer(h, w):
    a = normed(h)
    gate = jnp.dot(a, w["w_gate"], preferred_element_type=jnp.float32)
    up = jnp.dot(a, w["w_up"], preferred_element_type=jnp.float32)
    return h + matmul((jax.nn.silu(gate) * up).astype(jnp.bfloat16), w["w_down"])


def bit_of(me, stride):
    return lax.rem(lax.div(me, stride), 2)


def other(me, stride):
    return me + stride * (1 - 2 * bit_of(me, stride))


def all_reduce_kernel(shapes, n, *refs):
    k = len(shapes)
    grads, outs, sq_out = refs[:k], refs[k : 2 * k], refs[2 * k]
    refs = refs[2 * k + 1 :]
    own, landed, refs = refs[:k], [refs[k + 5 * i : k + 5 * i + 5] for i in range(k)], refs[6 * k :]
    final, sq, (local_sem, send_sem, recv_sem, ag_local, ag_send, ag_recv, sq_send, sq_recv) = refs[:k], refs[k], refs[k + 1 :]
    me = lax.axis_index("dp")
    core = bit_of(me, CORE)

    def remote(src, dst, send, recv, stride):
        return pltpu.make_async_remote_copy(src, dst, send, recv, device_id={"dp": other(me, stride)}, device_id_type=MESH)

    def columns(i, half):
        width = shapes[i][1] // 2
        return pl.ds(half * width, width)

    def starts(i, half):
        size, at = shapes[i][0] // 2, 0
        found = [at]
        for stride in ORDERS[half]:
            size //= 2
            at = at + bit_of(me, stride) * size
            found.append(at)
        return found

    def rs_copy(i, half, stage):
        stride = ORDERS[half][stage - 1]
        size = shapes[i][0] >> (stage + 1)
        at = starts(i, half)[stage - 1] + (1 - bit_of(me, stride)) * size
        cols = columns(i, half)
        return remote(
            own[i].at[pl.ds(pl.multiple_of(at, 16), size), cols],
            landed[i][stage].at[:, cols],
            send_sem.at[i, half, stage],
            recv_sem.at[i, half, stage],
            stride,
        )

    def core_copy(i):
        rows = shapes[i][0] // 2
        away = pl.ds(pl.multiple_of((1 - core) * rows, 16), rows)
        return remote(grads[i].at[away, :], landed[i][0], send_sem.at[i, 0, 0], recv_sem.at[i, 0, 0], CORE)

    def own_copy(i):
        rows = shapes[i][0] // 2
        return pltpu.make_async_copy(grads[i].at[pl.ds(pl.multiple_of(core * rows, 16), rows), :], own[i], local_sem.at[i])

    def summed(i, half, stage, at, row):
        cols, found = columns(i, half), starts(i, half)
        place = lambda start: pl.ds(pl.multiple_of(at - start + row, 16), 16)
        total = own[i][place(0), cols].astype(jnp.float32)
        for s in range(stage + 1):
            total += landed[i][s][place(found[s]), cols].astype(jnp.float32)
        return total

    def rs_step(i, half, stage):
        stride = ORDERS[half][stage - 1]
        size = shapes[i][0] >> (stage + 1)
        at = starts(i, half)[stage - 1] + (1 - bit_of(me, stride)) * size

        @pl.loop(0, size // 16)
        def _(block):
            row = block * 16
            total = summed(i, half, stage - 1, at, row)
            own[i][pl.ds(pl.multiple_of(at + row, 16), 16), columns(i, half)] = total.astype(jnp.bfloat16)

        rs_copy(i, half, stage).start()

    def finish(i, half):
        size, width = shapes[i][0] // 32, shapes[i][1] // 2
        at = starts(i, half)[4]

        @pl.loop(0, size // 16)
        def _(block):
            row = block * 16
            total = summed(i, half, 4, at, row).astype(jnp.bfloat16)
            final[i][pl.ds(pl.multiple_of(row, 16), 16), columns(i, half)] = total
            wide = total.astype(jnp.float32)
            wide = wide * wide
            part = wide[:, :128]
            for j in range(1, width // 128):
                part += wide[:, j * 128 : (j + 1) * 128]
            sq[...] += part

    def region(i, half, stage):
        size = shapes[i][0] >> (stage + 1)
        at = core * (shapes[i][0] // 2) + starts(i, half)[stage]
        return pl.ds(pl.multiple_of(at, 16), size), columns(i, half)

    def ag_copy(i, half, stage):
        rows, cols = region(i, half, stage)
        src = final[i].at[:, cols] if stage == 4 else outs[i].at[rows, cols]
        return remote(
            src, outs[i].at[rows, cols], ag_send.at[i, half, stage], ag_recv.at[i, half, stage], ORDERS[half][stage - 1]
        )

    def ag_own(i, half):
        rows, cols = region(i, half, 4)
        return pltpu.make_async_copy(final[i].at[:, cols], outs[i].at[rows, cols], ag_local.at[i, half])

    def ag_core(i):
        rows = shapes[i][0] // 2
        mine = pl.ds(pl.multiple_of(core * rows, 16), rows)
        return remote(outs[i].at[mine, :], outs[i].at[mine, :], ag_send.at[i, 0, 0], ag_recv.at[i, 0, 0], CORE)

    for i in range(k):
        core_copy(i).start()
        own_copy(i).start()
    sq[...] = jnp.zeros_like(sq)

    def advance(i, step):
        if step == 0:
            core_copy(i).wait_recv()
            own_copy(i).wait()
        if step < 4:
            for half in range(2):
                if step:
                    rs_copy(i, half, step).wait_recv()
                rs_step(i, half, step + 1)
        elif step == 4:
            for half in range(2):
                rs_copy(i, half, 4).wait_recv()
                finish(i, half)
                ag_copy(i, half, 4).start()
                ag_own(i, half).start()
        elif step < 8:
            for half in range(2):
                if step == 5:
                    ag_own(i, half).wait()
                ag_copy(i, half, 9 - step).wait_recv()
                ag_copy(i, half, 8 - step).start()
        elif step == 8:
            for half in range(2):
                ag_copy(i, half, 1).wait_recv()
            ag_core(i).start()
        else:
            ag_core(i).wait_recv()

    def sq_copy(away):
        to = lax.rem(me + away, n)
        return pltpu.make_async_remote_copy(
            sq, sq_out.at[me], sq_send.at[away], sq_recv.at[away], device_id={"dp": to}, device_id_type=MESH
        )

    for t in range(k + 9):
        for step in range(10):
            i = t - step
            if 0 <= i < k:
                advance(i, step)
                if step == 4 and i == k - 1:
                    sq_out[me] = sq[...]

                    @pl.loop(1, n)
                    def _(away):
                        sq_copy(away).start()

    @pl.loop(1, n)
    def _(away):
        sq_copy(away).wait()

    for i in range(k):
        core_copy(i).wait_send()
        ag_core(i).wait_send()
        for half in range(2):
            for stage in range(1, 5):
                rs_copy(i, half, stage).wait_send()
                ag_copy(i, half, stage).wait_send()


def all_reduce(grads, n):
    shapes, k = [g.shape for g in grads], len(grads)
    vmem = lambda rows, columns: pltpu.VMEM((rows, columns), jnp.bfloat16)
    scratch = [vmem(r // 2, c) for r, c in shapes]
    for r, c in shapes:
        scratch += [vmem(r >> (stage + 1), c) for stage in range(5)]
    scratch += [vmem(r // 32, c) for r, c in shapes]
    scratch += [pltpu.VMEM((16, 128), jnp.float32)]
    dma = pltpu.SemaphoreType.DMA
    scratch += [dma((k,)), dma((k, 2, 5)), dma((k, 2, 5)), dma((k, 2)), dma((k, 2, 5)), dma((k, 2, 5)), dma((n,)), dma((n,))]
    return pl.pallas_call(
        functools.partial(all_reduce_kernel, shapes, n),
        out_shape=[jax.ShapeDtypeStruct(g.shape, jnp.bfloat16) for g in grads]
        + [jax.ShapeDtypeStruct((n, 16, 128), jnp.float32)],
        in_specs=[pl.BlockSpec(memory_space=pl.ANY)] * k,
        out_specs=[pl.BlockSpec(memory_space=pl.ANY)] * k + [pl.BlockSpec(memory_space=pltpu.VMEM)],
        scratch_shapes=scratch,
        compiler_params=pltpu.CompilerParams(has_side_effects=True, vmem_limit_bytes=LIMIT),
        cost_estimate=pl.CostEstimate(flops=10**9, bytes_accessed=10**8, transcendentals=0),
        name="all_reduce",
    )(*grads)


def adamw_kernel(first, factor_ref, g0_ref, g1_ref, w_ref, m_ref, v_ref, w_out, m_out, v_out):
    factor = factor_ref[0, 0]

    def update(g_ref):
        g = g_ref[...].astype(jnp.float32) * factor
        m = 0.9 * m_ref[0] + 0.1 * g
        v = 0.95 * v_ref[0] + 0.05 * g * g
        w = w_ref[0].astype(jnp.float32)
        step = m * lax.rsqrt(v + 1e-8) + 0.1 * w
        w_out[0] = (w - 0.02 * step).astype(jnp.bfloat16)
        m_out[0] = m
        v_out[0] = v

    number = pl.program_id(0)

    @pl.when(number == 0)
    def _():
        update(g0_ref)

    @pl.when(number == 1)
    def _():
        update(g1_ref)


def adamw(factor, g0, g1, w, m, v, rows):
    layers, r, c = w.shape
    blocks = r // rows
    whole = pl.BlockSpec((1, rows, c), lambda number, i: (number, i, 0))
    in0 = pl.BlockSpec((rows, c), lambda number, i: (jnp.where(number == 0, i, blocks - 1), 0))
    in1 = pl.BlockSpec((rows, c), lambda number, i: (jnp.where(number == 1, i, 0), 0))
    return pl.pallas_call(
        functools.partial(adamw_kernel, 0),
        grid=(layers, blocks),
        out_shape=[jax.ShapeDtypeStruct(a.shape, a.dtype) for a in (w, m, v)],
        in_specs=[pl.BlockSpec((1, 1), lambda number, i: (0, 0), memory_space=pltpu.SMEM), in0, in1, whole, whole, whole],
        out_specs=[whole] * 3,
        compiler_params=pltpu.CompilerParams(vmem_limit_bytes=LIMIT, dimension_semantics=("arbitrary", "arbitrary")),
        cost_estimate=pl.CostEstimate(flops=20 * w.size, bytes_accessed=22 * w.size, transcendentals=w.size),
        name="adamw",
    )(factor, g0, g1, w, m, v)


def solution(mesh):
    n = mesh.shape["dp"]

    def step(x, dy, *arrays):
        weights, m, v = (arrays[i : i + 3] for i in (0, 3, 6))
        layers = weights[0].shape[0]
        h, kept = x[0], []
        for number in range(layers):
            kept.append(h)
            h = layer(h, {name: w[number] for name, w in zip(NAMES, weights, strict=True)})
        by_h, terms = dy[0], [None] * layers
        for number in reversed(range(layers)):
            _, back = jax.vjp(lambda w, h: layer(h, w), {name: w[number] for name, w in zip(NAMES, weights, strict=True)}, kept[number])
            by_w, by_h = back(by_h)
            terms[number] = [by_w[name] for name in NAMES]
        *summed, squares = all_reduce(terms[1] + terms[0], n)
        total = jnp.sum(squares)
        factor = jnp.minimum(1.0, 0.5 * lax.rsqrt(total / sum(w.size for w in weights) + 1e-30)).reshape(1, 1)
        pairs = zip(summed[3:], summed[:3], strict=True)
        new = [
            adamw(factor, *pair, w, m, v, rows)
            for pair, w, m, v, rows in zip(pairs, weights, m, v, (128, 128, 320), strict=True)
        ]
        return tuple(one[which] for which in range(3) for one in new)

    return jax.shard_map(
        step,
        mesh=mesh,
        in_specs=(P(("rep", "dp"), None, None),) * 2 + (P(None, None, None),) * 9,
        out_specs=(P("rep", None, None),) * 9,
        check_vma=False,
    )
```

```python
import functools

import jax
import jax.numpy as jnp
from jax import lax
from jax.experimental import pallas as pl
from jax.experimental.pallas import tpu as pltpu
from jax.sharding import PartitionSpec as P

MESH = pl.DeviceIdType.MESH
LIMIT = 66_000_000
CORE, Z1, Z2, Y, X = 1, 2, 4, 8, 16
ORDERS = ((X, Z1, Y, Z2), (Y, Z1, X, Z2))


def f32dot(a, w, over=0):
    return lax.dot_general(a, w, (((1,), (over,)), ((), ())), preferred_element_type=jnp.float32)


def normed(h):
    wide = h.astype(jnp.float32)
    scale = lax.rsqrt(jnp.mean(wide**2, -1, keepdims=True) + 1e-6)
    return (wide * scale).astype(jnp.bfloat16), scale


def bit_of(me, stride):
    return lax.rem(lax.div(me, stride), 2)


def other(me, stride):
    return me + stride * (1 - 2 * bit_of(me, stride))


ROWS, COLS, TOKENS, TILE = 1024, 2560, 2048, 512
TILES = COLS // TILE
HALF, WIDTH = ROWS // 2, COLS // 2


def gradients_kernel(which, n, *refs):
    k = len(which)
    count = max(which) + 1
    lhs, rhs, outs, sq_out = refs[:count], refs[count : count + k], refs[count + k : count + 2 * k], refs[count + 2 * k]
    refs = refs[count + 2 * k + 1 :]
    own, landed, refs = refs[:k], [refs[k + 5 * i : k + 5 * i + 5] for i in range(k)], refs[6 * k :]
    final, (sq, raw, turned, right, away) = refs[:k], refs[k : k + 5]
    raw_sem, right_sem, core_send, core_recv, send_sem, recv_sem, ag_local, ag_send, ag_recv, sq_send, sq_recv = refs[k + 5 :]
    me = lax.axis_index("dp")
    core = bit_of(me, CORE)

    def remote(src, dst, send, recv, stride):
        return pltpu.make_async_remote_copy(src, dst, send, recv, device_id={"dp": other(me, stride)}, device_id_type=MESH)

    def columns(half):
        return pl.ds(half * WIDTH, WIDTH)

    def starts(half):
        size, at = HALF, 0
        found = [at]
        for stride in ORDERS[half]:
            size //= 2
            at = at + bit_of(me, stride) * size
            found.append(at)
        return found

    def raw_copy(index):
        return pltpu.make_async_copy(lhs[index], raw, raw_sem)

    def right_copy(i, j):
        slot = lax.rem(i * TILES + j, 2)
        cols = pl.ds(pl.multiple_of(j * TILE, TILE), TILE)
        return pltpu.make_async_copy(rhs[i].at[:, cols], right.at[slot], right_sem.at[slot])

    def core_copy(i, j):
        cols = pl.ds(pl.multiple_of(j * TILE, TILE), TILE)
        return remote(away.at[lax.rem(j, 2)], landed[i][0].at[:, cols], core_send.at[i, j], core_recv.at[i, j], CORE)

    def rs_copy(i, half, stage):
        stride = ORDERS[half][stage - 1]
        size = ROWS >> (stage + 1)
        at = starts(half)[stage - 1] + (1 - bit_of(me, stride)) * size
        cols = columns(half)
        return remote(
            own[i].at[pl.ds(pl.multiple_of(at, 16), size), cols],
            landed[i][stage].at[:, cols],
            send_sem.at[i, half, stage],
            recv_sem.at[i, half, stage],
            stride,
        )

    def summed(i, half, stage, at, row):
        cols, found = columns(half), starts(half)
        place = lambda start: pl.ds(pl.multiple_of(at - start + row, 16), 16)
        total = own[i][place(0), cols].astype(jnp.float32)
        for s in range(stage + 1):
            total += landed[i][s][place(found[s]), cols].astype(jnp.float32)
        return total

    def rs_step(i, half, stage):
        stride = ORDERS[half][stage - 1]
        size = ROWS >> (stage + 1)
        at = starts(half)[stage - 1] + (1 - bit_of(me, stride)) * size

        @pl.loop(0, size // 16)
        def _(block):
            row = block * 16
            total = summed(i, half, stage - 1, at, row)
            own[i][pl.ds(pl.multiple_of(at + row, 16), 16), columns(half)] = total.astype(jnp.bfloat16)

        rs_copy(i, half, stage).start()

    def finish(i, half):
        at = starts(half)[4]

        @pl.loop(0, ROWS // 32 // 16)
        def _(block):
            row = block * 16
            total = summed(i, half, 4, at, row).astype(jnp.bfloat16)
            final[i][pl.ds(pl.multiple_of(row, 16), 16), columns(half)] = total
            wide = total.astype(jnp.float32)
            wide = wide * wide
            part = wide[:, :128]
            for j in range(1, WIDTH // 128):
                part += wide[:, j * 128 : (j + 1) * 128]
            sq[...] += part

    def region(half, stage):
        at = core * HALF + starts(half)[stage]
        return pl.ds(pl.multiple_of(at, 16), ROWS >> (stage + 1)), columns(half)

    def ag_copy(i, half, stage):
        rows, cols = region(half, stage)
        src = final[i].at[:, cols] if stage == 4 else outs[i].at[rows, cols]
        return remote(
            src, outs[i].at[rows, cols], ag_send.at[i, half, stage], ag_recv.at[i, half, stage], ORDERS[half][stage - 1]
        )

    def ag_own(i, half):
        rows, cols = region(half, 4)
        return pltpu.make_async_copy(final[i].at[:, cols], outs[i].at[rows, cols], ag_local.at[i, half])

    def ag_core(i):
        mine = pl.ds(pl.multiple_of(core * HALF, 16), HALF)
        return remote(outs[i].at[mine, :], outs[i].at[mine, :], ag_send.at[i, 0, 0], ag_recv.at[i, 0, 0], CORE)

    def advance(i, step):
        if step == 0:
            for j in range(TILES):
                core_copy(i, j).wait_recv()
        if step < 4:
            for half in range(2):
                if step:
                    rs_copy(i, half, step).wait_recv()
                rs_step(i, half, step + 1)
        elif step == 4:
            for half in range(2):
                rs_copy(i, half, 4).wait_recv()
                finish(i, half)
                ag_copy(i, half, 4).start()
                ag_own(i, half).start()
        elif step < 8:
            for half in range(2):
                if step == 5:
                    ag_own(i, half).wait()
                ag_copy(i, half, 9 - step).wait_recv()
                ag_copy(i, half, 8 - step).start()
        elif step == 8:
            for half in range(2):
                ag_copy(i, half, 1).wait_recv()
            ag_core(i).start()
        else:
            ag_core(i).wait_recv()

    def sq_copy(hops):
        to = lax.rem(me + hops, n)
        return pltpu.make_async_remote_copy(
            sq, sq_out.at[me], sq_send.at[hops], sq_recv.at[hops], device_id={"dp": to}, device_id_type=MESH
        )

    def turn():
        @pl.loop(0, TOKENS // 128)
        def _(block):
            at = pl.ds(pl.multiple_of(block * 128, 128), 128)
            turned[:, at] = raw[at, :].T

    def product(i, j):
        slot = lax.rem(i * TILES + j, 2)
        right_copy(i, j).wait()

        @pl.when(j + 1 < TILES)
        def _():
            right_copy(i, j + 1).start()

        if i + 1 < k:

            @pl.when(j + 1 == TILES)
            def _():
                right_copy(i + 1, 0).start()

        half = lambda which: turned[pl.ds(pl.multiple_of(which * HALF, HALF), HALF), :]
        dot = lambda a: jnp.dot(a, right[slot], preferred_element_type=jnp.float32).astype(jnp.bfloat16)
        away[lax.rem(j, 2)] = dot(half(1 - core))
        core_copy(i, j).start()
        own[i][:, pl.ds(pl.multiple_of(j * TILE, TILE), TILE)] = dot(half(core))

        @pl.when(j >= 1)
        def _():
            core_copy(i, j - 1).wait_send()

    def due(t):
        return [(t - 1 - step, step) for step in range(10) if 0 <= t - 1 - step < k]

    raw_copy(which[0]).start()
    right_copy(0, 0).start()
    sq[...] = jnp.zeros_like(sq)
    for t in range(k):
        if t == 0 or which[t] != which[t - 1]:
            raw_copy(which[t]).wait()
            turn()
            if which[t] + 1 < count:
                raw_copy(which[t] + 1).start()

        @pl.loop(0, TILES)
        def _(j):
            product(t, j)
            for place in range(TILES):
                some = [(i, step) for i, step in due(t) if step // 2 == place]
                if some:

                    @pl.when(j == place)
                    def _():
                        for i, step in some:
                            advance(i, step)

        core_copy(t, TILES - 1).wait_send()

    for t in range(k, k + 10):
        for i, step in due(t):
            advance(i, step)
            if step == 4 and i == k - 1:
                sq_out[me] = sq[...]

                @pl.loop(1, n)
                def _(hops):
                    sq_copy(hops).start()

    @pl.loop(1, n)
    def _(hops):
        sq_copy(hops).wait()

    for i in range(k):
        ag_core(i).wait_send()
        for half in range(2):
            for stage in range(1, 5):
                rs_copy(i, half, stage).wait_send()
                ag_copy(i, half, stage).wait_send()


def gradients(lhs, rhs, which, n):
    k = len(which)
    vmem = lambda *shape: pltpu.VMEM(shape, jnp.bfloat16)
    scratch = [vmem(HALF, COLS)] * k + [vmem(ROWS >> (stage + 1), COLS) for stage in range(5)] * k + [vmem(ROWS // 32, COLS)] * k
    scratch += [pltpu.VMEM((16, 128), jnp.float32), vmem(TOKENS, ROWS), vmem(ROWS, TOKENS), vmem(2, TOKENS, TILE), vmem(2, HALF, TILE)]
    dma = pltpu.SemaphoreType.DMA
    scratch += [dma, dma((2,)), dma((k, TILES)), dma((k, TILES)), dma((k, 2, 5)), dma((k, 2, 5))]
    scratch += [dma((k, 2)), dma((k, 2, 5)), dma((k, 2, 5)), dma((n,)), dma((n,))]
    return pl.pallas_call(
        functools.partial(gradients_kernel, which, n),
        out_shape=[jax.ShapeDtypeStruct((ROWS, COLS), jnp.bfloat16)] * k + [jax.ShapeDtypeStruct((n, 16, 128), jnp.float32)],
        in_specs=[pl.BlockSpec(memory_space=pl.ANY)] * (len(lhs) + k),
        out_specs=[pl.BlockSpec(memory_space=pl.ANY)] * k + [pl.BlockSpec(memory_space=pltpu.VMEM)],
        scratch_shapes=scratch,
        compiler_params=pltpu.CompilerParams(has_side_effects=True, vmem_limit_bytes=LIMIT),
        cost_estimate=pl.CostEstimate(flops=2 * k * TOKENS * ROWS * COLS, bytes_accessed=10**8, transcendentals=0),
        name="gradients",
    )(*lhs, *rhs)


def adamw_kernel(turned, factor_ref, g0_ref, g1_ref, w_ref, m_ref, v_ref, w_out, m_out, v_out):
    factor = factor_ref[0, 0]

    rows = w_ref.shape[1]
    strip = 128 if turned else 16

    def update(g_ref):
        @pl.loop(0, rows // strip)
        def _(block):
            at = pl.ds(pl.multiple_of(block * strip, strip), strip)
            g = (g_ref[:, at].astype(jnp.float32).T if turned else g_ref[at, :].astype(jnp.float32)) * factor
            m = 0.9 * m_ref[0, at] + 0.1 * g
            v = 0.95 * v_ref[0, at] + 0.05 * g * g
            w = w_ref[0, at].astype(jnp.float32)
            step = m * lax.rsqrt(v + 1e-8) + 0.1 * w
            w_out[0, at] = (w - 0.02 * step).astype(jnp.bfloat16)
            m_out[0, at] = m
            v_out[0, at] = v

    number = pl.program_id(0)

    @pl.when(number == 0)
    def _():
        update(g0_ref)

    @pl.when(number == 1)
    def _():
        update(g1_ref)


def adamw(factor, g0, g1, w, m, v, rows, turned):
    layers, r, c = w.shape
    blocks = r // rows
    whole = pl.BlockSpec((1, rows, c), lambda number, i: (number, i, 0))
    shape = (c, rows) if turned else (rows, c)
    at = lambda i: (0, i) if turned else (i, 0)
    in0 = pl.BlockSpec(shape, lambda number, i: at(jnp.where(number == 0, i, blocks - 1)))
    in1 = pl.BlockSpec(shape, lambda number, i: at(jnp.where(number == 1, i, 0)))
    return pl.pallas_call(
        functools.partial(adamw_kernel, turned),
        grid=(layers, blocks),
        out_shape=[jax.ShapeDtypeStruct(a.shape, a.dtype) for a in (w, m, v)],
        in_specs=[pl.BlockSpec((1, 1), lambda number, i: (0, 0), memory_space=pltpu.SMEM), in0, in1, whole, whole, whole],
        out_specs=[whole] * 3,
        compiler_params=pltpu.CompilerParams(vmem_limit_bytes=LIMIT, dimension_semantics=("arbitrary", "arbitrary")),
        cost_estimate=pl.CostEstimate(flops=20 * w.size, bytes_accessed=22 * w.size, transcendentals=w.size),
        name="adamw",
    )(factor, g0, g1, w, m, v)


def solution(mesh):
    n = mesh.shape["dp"]

    def step(x, dy, *arrays):
        weights, m, v = (arrays[i : i + 3] for i in (0, 3, 6))
        layers = weights[0].shape[0]
        (w_gate, w_up, w_down), kept = weights, []
        h = x[0]
        for number in range(layers):
            a, scale = normed(h)
            gate, up = f32dot(a, w_gate[number]), f32dot(a, w_up[number])
            kept.append((h, a, scale, gate, up))
            if number + 1 < layers:
                h = h + f32dot((jax.nn.silu(gate) * up).astype(jnp.bfloat16), w_down[number]).astype(jnp.bfloat16)
        by_h, lhs, rhs = dy[0], [], []
        for number in reversed(range(layers)):
            h, a, scale, gate, up = kept[number]
            by_act = f32dot(by_h, w_down[number], 1).astype(jnp.bfloat16).astype(jnp.float32)
            sig = jax.nn.sigmoid(gate)
            silu = gate * sig
            act = (silu * up).astype(jnp.bfloat16)
            by_up = (by_act * silu).astype(jnp.bfloat16)
            by_gate = (by_act * up * (sig + silu * (1 - sig))).astype(jnp.bfloat16)
            lhs += [by_h, a]
            rhs += [act, by_gate, by_up]
            if number:
                by_a = f32dot(by_gate, w_gate[number], 1) + f32dot(by_up, w_up[number], 1)
                by_a, wide = by_a.astype(jnp.bfloat16).astype(jnp.float32), h.astype(jnp.float32)
                by_scale = jnp.sum(by_a * wide, -1, keepdims=True)
                by_wide = by_a * scale - wide * (scale * scale * scale * by_scale / h.shape[-1])
                by_h = by_h + by_wide.astype(jnp.bfloat16)
        down1, gate1, up1, down0, gate0, up0, squares = gradients(lhs, rhs, (0, 1, 1, 2, 3, 3), n)
        total = jnp.sum(squares)
        factor = jnp.minimum(1.0, 0.5 * lax.rsqrt(total / sum(w.size for w in weights) + 1e-30)).reshape(1, 1)
        pairs = ((gate0, gate1), (up0, up1), (down0, down1))
        new = [
            adamw(factor, *pair, w, m, v, rows, turned)
            for pair, w, m, v, rows, turned in zip(pairs, weights, m, v, (256, 256, 640), (False, False, True), strict=True)
        ]
        return tuple(one[which] for which in range(3) for one in new)

    return jax.shard_map(
        step,
        mesh=mesh,
        in_specs=(P(("rep", "dp"), None, None),) * 2 + (P(None, None, None),) * 9,
        out_specs=(P("rep", None, None),) * 9,
        check_vma=False,
    )
```

```python
import functools

import jax
import jax.numpy as jnp
from jax import lax
from jax.experimental import pallas as pl
from jax.experimental.pallas import tpu as pltpu
from jax.sharding import PartitionSpec as P

MESH = pl.DeviceIdType.MESH
LIMIT = 66_000_000
CORE, Z1, Z2, Y, X = 1, 2, 4, 8, 16
ORDERS = ((X, Z1, Y, Z2), (Y, Z1, X, Z2))


def f32dot(a, w, over=0):
    return lax.dot_general(a, w, (((1,), (over,)), ((), ())), preferred_element_type=jnp.float32)


def scale_of(wide):
    return lax.rsqrt(jnp.mean(wide * wide, -1, keepdims=True) + 1e-6)


def bit_of(me, stride):
    return lax.rem(lax.div(me, stride), 2)


def other(me, stride):
    return me + stride * (1 - 2 * bit_of(me, stride))


ROWS, COLS, TOKENS, TILE = 1024, 2560, 2048, 512
TILES = COLS // TILE
HALF, WIDTH = ROWS // 2, COLS // 4


def gradients_kernel(which, n, *refs):
    k = len(which)
    units = [(i, c) for i in range(k) for c in range(2)]
    count = max(which) + 1
    lhs, rhs, outs, sq_out = refs[:count], refs[count : count + k], refs[count + k : count + 2 * k], refs[count + 2 * k]
    refs = refs[count + 2 * k + 1 :]
    own, landed, refs = refs[:k], [refs[k + 5 * i : k + 5 * i + 5] for i in range(k)], refs[6 * k :]
    final, (sq, raw, turned, right, away) = refs[:k], refs[k : k + 5]
    raw_sem, right_sem, core_send, core_recv, send_sem, recv_sem, ag_local, ag_send, ag_recv, sq_send, sq_recv = refs[k + 5 :]
    me = lax.axis_index("dp")
    core = bit_of(me, CORE)

    def remote(src, dst, send, recv, stride):
        return pltpu.make_async_remote_copy(src, dst, send, recv, device_id={"dp": other(me, stride)}, device_id_type=MESH)

    def columns(unit, half):
        return pl.ds(unit[1] * 2 * WIDTH + half * WIDTH, WIDTH)

    def starts(half):
        size, at = HALF, 0
        found = [at]
        for stride in ORDERS[half]:
            size //= 2
            at = at + bit_of(me, stride) * size
            found.append(at)
        return found

    def raw_copy(index):
        return pltpu.make_async_copy(lhs[index], raw, raw_sem)

    def right_copy(i, j):
        slot = lax.rem(i * TILES + j, 2)
        cols = pl.ds(pl.multiple_of(j * TILE, TILE), TILE)
        return pltpu.make_async_copy(rhs[i].at[:, cols], right.at[slot], right_sem.at[slot])

    def core_copy(i, j):
        cols = pl.ds(pl.multiple_of(j * TILE, TILE), TILE)
        return remote(away.at[lax.rem(j, 2)], landed[i][0].at[:, cols], core_send.at[i, j], core_recv.at[i, j], CORE)

    def rs_copy(unit, half, stage):
        stride = ORDERS[half][stage - 1]
        size = ROWS >> (stage + 1)
        at = starts(half)[stage - 1] + (1 - bit_of(me, stride)) * size
        cols = columns(unit, half)
        return remote(
            own[unit[0]].at[pl.ds(pl.multiple_of(at, 16), size), cols],
            landed[unit[0]][stage].at[:, cols],
            send_sem.at[units.index(unit), half, stage],
            recv_sem.at[units.index(unit), half, stage],
            stride,
        )

    def summed(unit, half, stage, at, row):
        cols, found = columns(unit, half), starts(half)
        place = lambda start: pl.ds(pl.multiple_of(at - start + row, 16), 16)
        total = own[unit[0]][place(0), cols].astype(jnp.float32)
        for s in range(stage + 1):
            total += landed[unit[0]][s][place(found[s]), cols].astype(jnp.float32)
        return total

    def rs_step(unit, half, stage):
        stride = ORDERS[half][stage - 1]
        size = ROWS >> (stage + 1)
        at = starts(half)[stage - 1] + (1 - bit_of(me, stride)) * size

        @pl.loop(0, size // 16)
        def _(block):
            row = block * 16
            total = summed(unit, half, stage - 1, at, row)
            own[unit[0]][pl.ds(pl.multiple_of(at + row, 16), 16), columns(unit, half)] = total.astype(jnp.bfloat16)

        rs_copy(unit, half, stage).start()

    def finish(unit, half):
        at = starts(half)[4]

        @pl.loop(0, ROWS // 32 // 16)
        def _(block):
            row = block * 16
            total = summed(unit, half, 4, at, row).astype(jnp.bfloat16)
            final[unit[0]][pl.ds(pl.multiple_of(row, 16), 16), columns(unit, half)] = total
            wide = total.astype(jnp.float32)
            wide = wide * wide
            part = wide[:, :128]
            for j in range(1, WIDTH // 128):
                part += wide[:, j * 128 : (j + 1) * 128]
            sq[...] += part

    def region(unit, half, stage):
        at = core * HALF + starts(half)[stage]
        return pl.ds(pl.multiple_of(at, 16), ROWS >> (stage + 1)), columns(unit, half)

    def ag_copy(unit, half, stage):
        rows, cols = region(unit, half, stage)
        src = final[unit[0]].at[:, cols] if stage == 4 else outs[unit[0]].at[rows, cols]
        return remote(
            src, outs[unit[0]].at[rows, cols], ag_send.at[units.index(unit), half, stage], ag_recv.at[units.index(unit), half, stage], ORDERS[half][stage - 1]
        )

    def ag_own(unit, half):
        rows, cols = region(unit, half, 4)
        return pltpu.make_async_copy(final[unit[0]].at[:, cols], outs[unit[0]].at[rows, cols], ag_local.at[units.index(unit), half])

    def ag_core(unit):
        mine, cols = pl.ds(pl.multiple_of(core * HALF, 16), HALF), pl.ds(unit[1] * 2 * WIDTH, 2 * WIDTH)
        place, number = outs[unit[0]].at[mine, cols], units.index(unit)
        return remote(place, place, ag_send.at[number, 0, 0], ag_recv.at[number, 0, 0], CORE)

    def advance(unit, step):
        if step == 0:
            for j in range(3) if unit[1] == 0 else range(3, TILES):
                core_copy(unit[0], j).wait_recv()
        if step < 4:
            for half in range(2):
                if step:
                    rs_copy(unit, half, step).wait_recv()
                rs_step(unit, half, step + 1)
        elif step == 4:
            for half in range(2):
                rs_copy(unit, half, 4).wait_recv()
                finish(unit, half)
                ag_copy(unit, half, 4).start()
                ag_own(unit, half).start()
        elif step < 8:
            for half in range(2):
                if step == 5:
                    ag_own(unit, half).wait()
                ag_copy(unit, half, 9 - step).wait_recv()
                ag_copy(unit, half, 8 - step).start()
        elif step == 8:
            for half in range(2):
                ag_copy(unit, half, 1).wait_recv()
            ag_core(unit).start()
        else:
            ag_core(unit).wait_recv()

    def sq_copy(hops):
        to = lax.rem(me + hops, n)
        return pltpu.make_async_remote_copy(
            sq, sq_out.at[me], sq_send.at[hops], sq_recv.at[hops], device_id={"dp": to}, device_id_type=MESH
        )

    def turn_lhs():
        @pl.loop(0, TOKENS // 128)
        def _(block):
            at = pl.ds(pl.multiple_of(block * 128, 128), 128)
            turned[:, at] = raw[at, :].T

    def product(i, j):
        slot = lax.rem(i * TILES + j, 2)
        right_copy(i, j).wait()

        @pl.when(j + 1 < TILES)
        def _():
            right_copy(i, j + 1).start()

        if i + 1 < k:

            @pl.when(j + 1 == TILES)
            def _():
                right_copy(i + 1, 0).start()

        half = lambda which: turned[pl.ds(pl.multiple_of(which * HALF, HALF), HALF), :]
        dot = lambda a: jnp.dot(a, right[slot], preferred_element_type=jnp.float32).astype(jnp.bfloat16)
        away[lax.rem(j, 2)] = dot(half(1 - core))
        core_copy(i, j).start()
        own[i][:, pl.ds(pl.multiple_of(j * TILE, TILE), TILE)] = dot(half(core))

        @pl.when(j >= 1)
        def _():
            core_copy(i, j - 1).wait_send()

    def due(turn):
        return [(units[turn - 1 - step], step) for step in range(10) if 0 <= turn - 1 - step < len(units)]

    def share(some, part, parts):
        size = -(-len(some) // parts)
        return some[part * size : (part + 1) * size]

    raw_copy(which[0]).start()
    right_copy(0, 0).start()
    sq[...] = jnp.zeros_like(sq)
    for t in range(k):
        if t == 0 or which[t] != which[t - 1]:
            raw_copy(which[t]).wait()
            turn_lhs()
            if which[t] + 1 < count:
                raw_copy(which[t] + 1).start()

        @pl.loop(0, TILES)
        def _(j):
            product(t, j)
            for place in range(TILES):
                some = share(due(2 * t), place, 3) if place < 3 else share(due(2 * t + 1), place - 3, 2)
                if some:

                    @pl.when(j == place)
                    def _():
                        for unit, step in some:
                            advance(unit, step)

        core_copy(t, TILES - 1).wait_send()

    for turn in range(2 * k, 2 * k + 10):
        for unit, step in due(turn):
            advance(unit, step)
            if step == 4 and unit == units[-1]:
                sq_out[me] = sq[...]

                @pl.loop(1, n)
                def _(hops):
                    sq_copy(hops).start()

    @pl.loop(1, n)
    def _(hops):
        sq_copy(hops).wait()

    for unit in units:
        ag_core(unit).wait_send()
        for half in range(2):
            for stage in range(1, 5):
                rs_copy(unit, half, stage).wait_send()
                ag_copy(unit, half, stage).wait_send()


def gradients(lhs, rhs, which, n):
    k = len(which)
    vmem = lambda *shape: pltpu.VMEM(shape, jnp.bfloat16)
    scratch = [vmem(HALF, COLS)] * k + [vmem(ROWS >> (stage + 1), COLS) for stage in range(5)] * k + [vmem(ROWS // 32, COLS)] * k
    scratch += [pltpu.VMEM((16, 128), jnp.float32), vmem(TOKENS, ROWS), vmem(ROWS, TOKENS), vmem(2, TOKENS, TILE), vmem(2, HALF, TILE)]
    dma = pltpu.SemaphoreType.DMA
    scratch += [dma, dma((2,)), dma((k, TILES)), dma((k, TILES)), dma((2 * k, 2, 5)), dma((2 * k, 2, 5))]
    scratch += [dma((2 * k, 2)), dma((2 * k, 2, 5)), dma((2 * k, 2, 5)), dma((n,)), dma((n,))]
    return pl.pallas_call(
        functools.partial(gradients_kernel, which, n),
        out_shape=[jax.ShapeDtypeStruct((ROWS, COLS), jnp.bfloat16)] * k + [jax.ShapeDtypeStruct((n, 16, 128), jnp.float32)],
        in_specs=[pl.BlockSpec(memory_space=pl.ANY)] * (len(lhs) + k),
        out_specs=[pl.BlockSpec(memory_space=pl.ANY)] * k + [pl.BlockSpec(memory_space=pltpu.VMEM)],
        scratch_shapes=scratch,
        compiler_params=pltpu.CompilerParams(has_side_effects=True, vmem_limit_bytes=LIMIT),
        cost_estimate=pl.CostEstimate(flops=2 * k * TOKENS * ROWS * COLS, bytes_accessed=10**8, transcendentals=0),
        name="gradients",
    )(*lhs, *rhs)


PART, CHUNK, STRIP = 512, 512, 256
PARTS = COLS // PART
CHUNKS = [pl.ds(r * CHUNK, CHUNK) for r in range(TOKENS // CHUNK)]


def forward_kernel(x_hbm, w_gate, w_up, w_down, gate_out, up_out, act_out, a_hbm, h_hbm, next_hbm, h, a, total, sem):
    j = pl.program_id(0)
    keep_a = pltpu.make_async_copy(a, a_hbm, sem.at[1])

    @pl.when(j == 0)
    def _():
        load = pltpu.make_async_copy(x_hbm, h, sem.at[0])
        load.start()
        load.wait()
        total[...] = jnp.zeros_like(total)

        @pl.loop(0, TOKENS // STRIP)
        def _(block):
            rows = pl.ds(pl.multiple_of(block * STRIP, STRIP), STRIP)
            wide = h[rows, :].astype(jnp.float32)
            a[rows, :] = (wide * scale_of(wide)).astype(jnp.bfloat16)

        keep_a.start()

    for rows in CHUNKS:
        gate, up = f32dot(a[rows, :], w_gate[...]), f32dot(a[rows, :], w_up[...])
        act = (gate * jax.nn.sigmoid(gate) * up).astype(jnp.bfloat16)
        gate_out[rows, :] = gate
        up_out[rows, :] = up
        act_out[rows, :] = act
        total[rows, :] += f32dot(act, w_down[...])

    @pl.when(j == PARTS - 1)
    def _():
        keep_a.wait()

        @pl.loop(0, TOKENS // STRIP)
        def _(block):
            rows = pl.ds(pl.multiple_of(block * STRIP, STRIP), STRIP)
            new = h[rows, :] + total[rows, :].astype(jnp.bfloat16)
            h[rows, :] = new
            wide = new.astype(jnp.float32)
            a[rows, :] = (wide * scale_of(wide)).astype(jnp.bfloat16)

        copies = [pltpu.make_async_copy(h, h_hbm, sem.at[0]), pltpu.make_async_copy(a, next_hbm, sem.at[1])]
        for copy in copies:
            copy.start()
        for copy in copies:
            copy.wait()


def hidden_gradients(gate, up, by_act):
    by_act = by_act.astype(jnp.bfloat16).astype(jnp.float32)
    sig = jax.nn.sigmoid(gate)
    silu = gate * sig
    by_gate = by_act * up * (sig + silu * (1 - sig))
    return (silu * up).astype(jnp.bfloat16), by_gate.astype(jnp.bfloat16), (by_act * silu).astype(jnp.bfloat16)


def top_kernel(
    a_hbm, by_hbm, h_hbm, w_gate, w_up, w_down, act_out, by_gate_out, by_up_out, by_h_hbm, a, by, h, total, sem
):
    j = pl.program_id(0)
    load_h = pltpu.make_async_copy(h_hbm, h, sem.at[2])

    @pl.when(j == 0)
    def _():
        loads = [pltpu.make_async_copy(a_hbm, a, sem.at[0]), pltpu.make_async_copy(by_hbm, by, sem.at[1])]
        for load in loads:
            load.start()
        load_h.start()
        total[...] = jnp.zeros_like(total)
        for load in loads:
            load.wait()

    for rows in CHUNKS:
        gate, up = f32dot(a[rows, :], w_gate[...]), f32dot(a[rows, :], w_up[...])
        act, by_gate, by_up = hidden_gradients(gate, up, f32dot(by[rows, :], w_down[...], 1))
        act_out[rows, :] = act
        by_gate_out[rows, :] = by_gate
        by_up_out[rows, :] = by_up
        total[rows, :] += f32dot(by_gate, w_gate[...], 1) + f32dot(by_up, w_up[...], 1)

    @pl.when(j == PARTS - 1)
    def _():
        load_h.wait()

        @pl.loop(0, TOKENS // STRIP)
        def _(block):
            rows = pl.ds(pl.multiple_of(block * STRIP, STRIP), STRIP)
            by_a = total[rows, :].astype(jnp.bfloat16).astype(jnp.float32)
            wide = h[rows, :].astype(jnp.float32)
            scale = scale_of(wide)
            by_scale = jnp.sum(by_a * wide, -1, keepdims=True)
            by_wide = by_a * scale - wide * (scale * scale * scale * by_scale * (1 / ROWS))
            by[rows, :] = by[rows, :] + by_wide.astype(jnp.bfloat16)

        store = pltpu.make_async_copy(by, by_h_hbm, sem.at[0])
        store.start()
        store.wait()


def bottom_kernel(by, w_down, gate, up, by_gate_out, by_up_out):
    for rows in CHUNKS:
        _, by_gate, by_up = hidden_gradients(gate[rows, :], up[rows, :], f32dot(by[rows, :], w_down[...], 1))
        by_gate_out[rows, :] = by_gate
        by_up_out[rows, :] = by_up


def wide_part(number):
    return pl.BlockSpec((None, ROWS, PART), lambda j: (number, 0, j))


def tall_part(number):
    return pl.BlockSpec((None, PART, ROWS), lambda j: (number, j, 0))


ANY = pl.BlockSpec(memory_space=pl.ANY)
HIDDEN = pl.BlockSpec((TOKENS, PART), lambda j: (0, j))


def layer_call(kernel, matmuls, in_specs, out_specs, outs, scratch, name):
    return pl.pallas_call(
        kernel,
        grid=(PARTS,),
        out_shape=[jax.ShapeDtypeStruct(shape, dtype) for shape, dtype in outs],
        in_specs=in_specs,
        out_specs=out_specs,
        scratch_shapes=scratch,
        compiler_params=pltpu.CompilerParams(vmem_limit_bytes=LIMIT, dimension_semantics=("arbitrary",)),
        cost_estimate=pl.CostEstimate(flops=2 * matmuls * TOKENS * ROWS * COLS, bytes_accessed=10**8, transcendentals=TOKENS * COLS),
        name=name,
    )


def forward(x, w_gate, w_up, w_down):
    tokens, hidden = (TOKENS, ROWS), (TOKENS, COLS)
    outs = [(hidden, jnp.float32)] * 2 + [(hidden, jnp.bfloat16)] + [(tokens, jnp.bfloat16)] * 3
    scratch = [pltpu.VMEM(tokens, jnp.bfloat16)] * 2 + [pltpu.VMEM(tokens, jnp.float32), pltpu.SemaphoreType.DMA((2,))]
    specs = [ANY, wide_part(0), wide_part(0), tall_part(0)], [HIDDEN] * 3 + [ANY] * 3
    return layer_call(forward_kernel, 3, *specs, outs, scratch, "forward")(x, w_gate, w_up, w_down)


def top(a, by, h, w_gate, w_up, w_down):
    tokens, hidden = (TOKENS, ROWS), (TOKENS, COLS)
    outs = [(hidden, jnp.bfloat16)] * 3 + [(tokens, jnp.bfloat16)]
    scratch = [pltpu.VMEM(tokens, jnp.bfloat16)] * 3 + [pltpu.VMEM(tokens, jnp.float32), pltpu.SemaphoreType.DMA((3,))]
    specs = [ANY] * 3 + [wide_part(1), wide_part(1), tall_part(1)], [HIDDEN] * 3 + [ANY]
    return layer_call(top_kernel, 5, *specs, outs, scratch, "top")(a, by, h, w_gate, w_up, w_down)


def bottom(by, w_down, gate, up):
    outs = [((TOKENS, COLS), jnp.bfloat16)] * 2
    whole = pl.BlockSpec((TOKENS, ROWS), lambda j: (0, 0))
    return layer_call(bottom_kernel, 1, [whole, tall_part(0), HIDDEN, HIDDEN], [HIDDEN] * 2, outs, [], "bottom")(by, w_down, gate, up)


def adamw_kernel(turned, factor_ref, g0_ref, g1_ref, w_ref, m_ref, v_ref, w_out, m_out, v_out):
    factor = factor_ref[0, 0]

    rows = w_ref.shape[1]
    strip = 128 if turned else 16

    def update(g_ref):
        @pl.loop(0, rows // strip)
        def _(block):
            at = pl.ds(pl.multiple_of(block * strip, strip), strip)
            g = (g_ref[:, at].astype(jnp.float32).T if turned else g_ref[at, :].astype(jnp.float32)) * factor
            m = 0.9 * m_ref[0, at] + 0.1 * g
            v = 0.95 * v_ref[0, at] + 0.05 * g * g
            w = w_ref[0, at].astype(jnp.float32)
            step = m * lax.rsqrt(v + 1e-8) + 0.1 * w
            w_out[0, at] = (w - 0.02 * step).astype(jnp.bfloat16)
            m_out[0, at] = m
            v_out[0, at] = v

    number = pl.program_id(0)

    @pl.when(number == 0)
    def _():
        update(g0_ref)

    @pl.when(number == 1)
    def _():
        update(g1_ref)


def adamw(factor, g0, g1, w, m, v, rows, turned):
    layers, r, c = w.shape
    blocks = r // rows
    whole = pl.BlockSpec((1, rows, c), lambda number, i: (number, i, 0))
    shape = (c, rows) if turned else (rows, c)
    at = lambda i: (0, i) if turned else (i, 0)
    in0 = pl.BlockSpec(shape, lambda number, i: at(jnp.where(number == 0, i, blocks - 1)))
    in1 = pl.BlockSpec(shape, lambda number, i: at(jnp.where(number == 1, i, 0)))
    return pl.pallas_call(
        functools.partial(adamw_kernel, turned),
        grid=(layers, blocks),
        out_shape=[jax.ShapeDtypeStruct(a.shape, a.dtype) for a in (w, m, v)],
        in_specs=[pl.BlockSpec((1, 1), lambda number, i: (0, 0), memory_space=pltpu.SMEM), in0, in1, whole, whole, whole],
        out_specs=[whole] * 3,
        compiler_params=pltpu.CompilerParams(vmem_limit_bytes=LIMIT, dimension_semantics=("arbitrary", "arbitrary")),
        cost_estimate=pl.CostEstimate(flops=20 * w.size, bytes_accessed=22 * w.size, transcendentals=w.size),
        name="adamw",
    )(factor, g0, g1, w, m, v)


def solution(mesh):
    n = mesh.shape["dp"]

    def step(x, dy, *arrays):
        weights, m, v = (arrays[i : i + 3] for i in (0, 3, 6))
        gate, up, act0, a0, h1, a1 = forward(x[0], *weights)
        act1, by_gate1, by_up1, by_h1 = top(a1, dy[0], h1, *weights)
        by_gate0, by_up0 = bottom(by_h1, weights[2], gate, up)
        lhs, rhs = (dy[0], a1, by_h1, a0), (act1, by_gate1, by_up1, act0, by_gate0, by_up0)
        down1, gate1, up1, down0, gate0, up0, squares = gradients(lhs, rhs, (0, 1, 1, 2, 3, 3), n)
        total = jnp.sum(squares)
        factor = jnp.minimum(1.0, 0.5 * lax.rsqrt(total / sum(w.size for w in weights) + 1e-30)).reshape(1, 1)
        pairs = ((gate0, gate1), (up0, up1), (down0, down1))
        new = [
            adamw(factor, *pair, w, m, v, rows, turned)
            for pair, w, m, v, rows, turned in zip(pairs, weights, m, v, (256, 256, 640), (False, False, True), strict=True)
        ]
        return tuple(one[which] for which in range(3) for one in new)

    return jax.shard_map(
        step,
        mesh=mesh,
        in_specs=(P(("rep", "dp"), None, None),) * 2 + (P(None, None, None),) * 9,
        out_specs=(P("rep", None, None),) * 9,
        check_vma=False,
    )
```

```python
import functools

import jax
import jax.numpy as jnp
from jax import lax
from jax.experimental import pallas as pl
from jax.experimental.pallas import tpu as pltpu
from jax.sharding import PartitionSpec as P

MESH = pl.DeviceIdType.MESH
LIMIT = 67_000_000
CORE, Z1, Z2, Y, X = 1, 2, 4, 8, 16
ORDERS = ((X, Z1, Y, Z2), (Y, Z1, X, Z2))


def f32dot(a, w, over=0):
    return lax.dot_general(a, w, (((1,), (over,)), ((), ())), preferred_element_type=jnp.float32)


def scale_of(wide):
    return lax.rsqrt(jnp.mean(wide * wide, -1, keepdims=True) + 1e-6)


def bit_of(me, stride):
    return lax.rem(lax.div(me, stride), 2)


def other(me, stride):
    return me + stride * (1 - 2 * bit_of(me, stride))


ROWS, COLS, TOKENS, TILE = 1024, 2560, 2048, 512
TILES = COLS // TILE
HALF, WIDTH = ROWS // 2, COLS // 4
LATE, LATE_ROWS = 4, 256
CHUNKS_LATE = TOKENS // LATE_ROWS


def gradients_kernel(which, n, *refs):
    k = len(which)
    units = [(i, c) for i in range(k) for c in range(2)]
    count = max(which) + 1
    lhs, rhs, (gates, ups, w_down), refs = refs[:count], refs[count : count + k - 2], refs[count + k - 2 : count + k + 1], refs[count + k + 1 :]
    outs, sq_out, by_hidden, refs = refs[:k], refs[k], refs[k + 1 : k + 3], refs[k + 3 :]
    rhs += by_hidden
    own, landed, refs = refs[:k], [refs[k + 5 * i : k + 5 * i + 5] for i in range(k)], refs[6 * k :]
    final, (sq, raw, turned, right, away, projected) = refs[:k], refs[k : k + 6]
    raw_sem, right_sem, core_send, core_recv, send_sem, recv_sem, ag_local, ag_send, ag_recv, sq_send, sq_recv = refs[k + 6 : k + 17]
    w_sem, in_sem, out_sem = refs[k + 17 :]
    me = lax.axis_index("dp")
    core = bit_of(me, CORE)

    def remote(src, dst, send, recv, stride):
        return pltpu.make_async_remote_copy(src, dst, send, recv, device_id={"dp": other(me, stride)}, device_id_type=MESH)

    def columns(unit, half):
        return pl.ds(unit[1] * 2 * WIDTH + half * WIDTH, WIDTH)

    def starts(half):
        size, at = HALF, 0
        found = [at]
        for stride in ORDERS[half]:
            size //= 2
            at = at + bit_of(me, stride) * size
            found.append(at)
        return found

    def raw_copy(index):
        return pltpu.make_async_copy(lhs[index], raw, raw_sem)

    def right_copy(i, j):
        slot = lax.rem(i * TILES + j, 2)
        cols = pl.ds(pl.multiple_of(j * TILE, TILE), TILE)
        return pltpu.make_async_copy(rhs[i].at[:, cols], right.at[slot], right_sem.at[slot])

    def core_copy(i, j):
        cols = pl.ds(pl.multiple_of(j * TILE, TILE), TILE)
        return remote(away.at[lax.rem(j, 2)], landed[i][0].at[:, cols], core_send.at[i, j], core_recv.at[i, j], CORE)

    def rs_copy(unit, half, stage):
        stride = ORDERS[half][stage - 1]
        size = ROWS >> (stage + 1)
        at = starts(half)[stage - 1] + (1 - bit_of(me, stride)) * size
        cols = columns(unit, half)
        return remote(
            own[unit[0]].at[pl.ds(pl.multiple_of(at, 16), size), cols],
            landed[unit[0]][stage].at[:, cols],
            send_sem.at[units.index(unit), half, stage],
            recv_sem.at[units.index(unit), half, stage],
            stride,
        )

    def summed(unit, half, stage, at, row):
        cols, found = columns(unit, half), starts(half)
        place = lambda start: pl.ds(pl.multiple_of(at - start + row, 16), 16)
        total = own[unit[0]][place(0), cols].astype(jnp.float32)
        for s in range(stage + 1):
            total += landed[unit[0]][s][place(found[s]), cols].astype(jnp.float32)
        return total

    def rs_step(unit, half, stage):
        stride = ORDERS[half][stage - 1]
        size = ROWS >> (stage + 1)
        at = starts(half)[stage - 1] + (1 - bit_of(me, stride)) * size

        @pl.loop(0, size // 16)
        def _(block):
            row = block * 16
            total = summed(unit, half, stage - 1, at, row)
            own[unit[0]][pl.ds(pl.multiple_of(at + row, 16), 16), columns(unit, half)] = total.astype(jnp.bfloat16)

        rs_copy(unit, half, stage).start()

    def finish(unit, half):
        at = starts(half)[4]

        @pl.loop(0, ROWS // 32 // 16)
        def _(block):
            row = block * 16
            total = summed(unit, half, 4, at, row).astype(jnp.bfloat16)
            final[unit[0]][pl.ds(pl.multiple_of(row, 16), 16), columns(unit, half)] = total
            wide = total.astype(jnp.float32)
            wide = wide * wide
            part = wide[:, :128]
            for j in range(1, WIDTH // 128):
                part += wide[:, j * 128 : (j + 1) * 128]
            sq[...] += part

    def region(unit, half, stage):
        at = core * HALF + starts(half)[stage]
        return pl.ds(pl.multiple_of(at, 16), ROWS >> (stage + 1)), columns(unit, half)

    def ag_copy(unit, half, stage):
        rows, cols = region(unit, half, stage)
        src = final[unit[0]].at[:, cols] if stage == 4 else outs[unit[0]].at[rows, cols]
        return remote(
            src, outs[unit[0]].at[rows, cols], ag_send.at[units.index(unit), half, stage], ag_recv.at[units.index(unit), half, stage], ORDERS[half][stage - 1]
        )

    def ag_own(unit, half):
        rows, cols = region(unit, half, 4)
        return pltpu.make_async_copy(final[unit[0]].at[:, cols], outs[unit[0]].at[rows, cols], ag_local.at[units.index(unit), half])

    def ag_core(unit):
        mine, cols = pl.ds(pl.multiple_of(core * HALF, 16), HALF), pl.ds(unit[1] * 2 * WIDTH, 2 * WIDTH)
        place, number = outs[unit[0]].at[mine, cols], units.index(unit)
        return remote(place, place, ag_send.at[number, 0, 0], ag_recv.at[number, 0, 0], CORE)

    def advance(unit, step):
        if step == 0:
            for j in range(3) if unit[1] == 0 else range(3, TILES):
                core_copy(unit[0], j).wait_recv()
        if step < 4:
            for half in range(2):
                if step:
                    rs_copy(unit, half, step).wait_recv()
                rs_step(unit, half, step + 1)
        elif step == 4:
            for half in range(2):
                rs_copy(unit, half, 4).wait_recv()
                finish(unit, half)
                ag_copy(unit, half, 4).start()
                ag_own(unit, half).start()
        elif step < 8:
            for half in range(2):
                if step == 5:
                    ag_own(unit, half).wait()
                ag_copy(unit, half, 9 - step).wait_recv()
                ag_copy(unit, half, 8 - step).start()
        elif step == 8:
            for half in range(2):
                ag_copy(unit, half, 1).wait_recv()
            ag_core(unit).start()
        else:
            ag_core(unit).wait_recv()

    def sq_copy(hops):
        to = lax.rem(me + hops, n)
        return pltpu.make_async_remote_copy(
            sq, sq_out.at[me], sq_send.at[hops], sq_recv.at[hops], device_id={"dp": to}, device_id_type=MESH
        )

    def turn_lhs():
        @pl.loop(0, TOKENS // 128)
        def _(block):
            at = pl.ds(pl.multiple_of(block * 128, 128), 128)
            turned[:, at] = raw[at, :].T

    def product(i, j):
        slot = lax.rem(i * TILES + j, 2)
        right_copy(i, j).wait()

        @pl.when(j + 1 < TILES)
        def _():
            right_copy(i, j + 1).start()

        if i + 1 < k and i + 1 != LATE:

            @pl.when(j + 1 == TILES)
            def _():
                right_copy(i + 1, 0).start()

        half = lambda which: turned[pl.ds(pl.multiple_of(which * HALF, HALF), HALF), :]
        dot = lambda a: jnp.dot(a, right[slot], preferred_element_type=jnp.float32).astype(jnp.bfloat16)
        away[lax.rem(j, 2)] = dot(half(1 - core))
        core_copy(i, j).start()
        own[i][:, pl.ds(pl.multiple_of(j * TILE, TILE), TILE)] = dot(half(core))

        @pl.when(j >= 1)
        def _():
            core_copy(i, j - 1).wait_send()

    def w_copies(part):
        slot, rows = lax.rem(part, 2), pl.ds(pl.multiple_of(part * TILE, TILE), TILE)
        return [
            pltpu.make_async_copy(
                w_down.at[0, rows, pl.ds(d * TILE, TILE)], right.at[slot, pl.ds(d * TILE, TILE), :], w_sem.at[slot, d]
            )
            for d in range(ROWS // TILE)
        ]

    def place_of(q):
        part, chunk = lax.div(q, CHUNKS_LATE), lax.rem(q, CHUNKS_LATE)
        return pl.ds(pl.multiple_of(chunk * LATE_ROWS, LATE_ROWS), LATE_ROWS), pl.ds(pl.multiple_of(part * TILE, TILE), TILE)

    def in_copies(q):
        slot, place = lax.rem(q, 2), place_of(q)
        return [pltpu.make_async_copy(ref.at[place], projected.at[slot, d], in_sem.at[slot, d]) for d, ref in enumerate((gates, ups))]

    def out_copies(q):
        slot, place = lax.rem(q, 2), place_of(q)
        return [
            pltpu.make_async_copy(away.at[slot, pl.ds(d * LATE_ROWS, LATE_ROWS), :], ref.at[place], out_sem.at[slot, d])
            for d, ref in enumerate(by_hidden)
        ]

    def start(copies):
        for copy in copies:
            copy.start()

    def wait(copies):
        for copy in copies:
            copy.wait()

    def late(q, number):
        part, chunk, slot = lax.div(q, CHUNKS_LATE), lax.rem(q, CHUNKS_LATE), lax.rem(q, 2)
        wait(in_copies(q))

        @pl.when(q + 1 < number)
        def _():
            start(in_copies(q + 1))

        @pl.when(chunk == 0)
        def _():
            wait(w_copies(part))

            @pl.when(part + 1 < TILES)
            def _():
                start(w_copies(part + 1))

        @pl.when(q >= 2)
        def _():
            wait(out_copies(q - 2))

        rows = pl.ds(pl.multiple_of(chunk * LATE_ROWS, LATE_ROWS), LATE_ROWS)
        w = right.at[lax.rem(part, 2)]
        for side in range(2):
            cols = pl.ds(side * (TILE // 2), TILE // 2)
            by_act = sum(
                f32dot(raw[rows, pl.ds(d * TILE, TILE)], w[pl.ds(d * TILE + side * (TILE // 2), TILE // 2), :], 1)
                for d in range(ROWS // TILE)
            )
            _, by_gate, by_up = hidden_gradients(projected[slot, 0, :, cols], projected[slot, 1, :, cols], by_act)
            away[slot, pl.ds(0, LATE_ROWS), cols] = by_gate
            away[slot, pl.ds(LATE_ROWS, LATE_ROWS), cols] = by_up
        start(out_copies(q))

    def late_phase(first, second):
        number = TILES * CHUNKS_LATE
        start(w_copies(0))
        start(in_copies(0))

        @pl.loop(0, number)
        def _(q):
            late(q, number)
            for place, some in [(part * number // 6, share(first, part, 3)) for part in range(3)] + [
                ((part + 3) * number // 6, share(second, part, 3)) for part in range(3)
            ]:
                if some:

                    @pl.when(q == place)
                    def _():
                        for unit, step in some:
                            advance(unit, step)

        wait(out_copies(number - 2))
        wait(out_copies(number - 1))

    def due(turn):
        ready = [u + 1 + 2 * (u >= 2 * LATE) for u in range(len(units))]
        return [(units[u], turn - ready[u]) for u in reversed(range(len(units))) if 0 <= turn - ready[u] < 10]

    def share(some, part, parts):
        size = -(-len(some) // parts)
        return some[part * size : (part + 1) * size]

    raw_copy(which[0]).start()
    right_copy(0, 0).start()
    sq[...] = jnp.zeros_like(sq)
    for t in range(k):
        turn = 2 * t + 2 * (t >= LATE)
        if t == LATE:
            late_phase(due(turn - 2), due(turn - 1))
            raw_copy(which[t]).start()
            right_copy(t, 0).start()
        if t == 0 or which[t] != which[t - 1]:
            raw_copy(which[t]).wait()
            turn_lhs()
            if which[t] + 1 < count and t + 1 != LATE:
                raw_copy(which[t] + 1).start()

        @pl.loop(0, TILES)
        def _(j):
            product(t, j)
            for place in range(TILES):
                some = share(due(turn), place, 3) if place < 3 else share(due(turn + 1), place - 3, 2)
                if some:

                    @pl.when(j == place)
                    def _():
                        for unit, step in some:
                            advance(unit, step)

        core_copy(t, TILES - 1).wait_send()

    for turn in range(2 * k + 2, 2 * k + 12):
        for unit, step in due(turn):
            advance(unit, step)
            if step == 4 and unit == units[-1]:
                sq_out[me] = sq[...]

                @pl.loop(1, n)
                def _(hops):
                    sq_copy(hops).start()

    @pl.loop(1, n)
    def _(hops):
        sq_copy(hops).wait()

    for unit in units:
        ag_core(unit).wait_send()
        for half in range(2):
            for stage in range(1, 5):
                rs_copy(unit, half, stage).wait_send()
                ag_copy(unit, half, stage).wait_send()


def gradients(lhs, rhs, gate, up, w_down, which, n):
    k = len(which)
    vmem = lambda *shape: pltpu.VMEM(shape, jnp.bfloat16)
    scratch = [vmem(HALF, COLS)] * k + [vmem(ROWS >> (stage + 1), COLS) for stage in range(5)] * k + [vmem(ROWS // 32, COLS)] * k
    scratch += [pltpu.VMEM((16, 128), jnp.float32), vmem(TOKENS, ROWS), vmem(ROWS, TOKENS), vmem(2, TOKENS, TILE), vmem(2, HALF, TILE)]
    scratch += [pltpu.VMEM((2, 2, LATE_ROWS, TILE), jnp.float32)]
    dma = pltpu.SemaphoreType.DMA
    scratch += [dma, dma((2,)), dma((k, TILES)), dma((k, TILES)), dma((2 * k, 2, 5)), dma((2 * k, 2, 5))]
    scratch += [dma((2 * k, 2)), dma((2 * k, 2, 5)), dma((2 * k, 2, 5)), dma((n,)), dma((n,))]
    scratch += [dma((2, 2)), dma((2, 2)), dma((2, 2))]
    return pl.pallas_call(
        functools.partial(gradients_kernel, which, n),
        out_shape=[jax.ShapeDtypeStruct((ROWS, COLS), jnp.bfloat16)] * k + [jax.ShapeDtypeStruct((n, 16, 128), jnp.float32)]
        + [jax.ShapeDtypeStruct((TOKENS, COLS), jnp.bfloat16)] * 2,
        in_specs=[pl.BlockSpec(memory_space=pl.ANY)] * (len(lhs) + k + 1),
        out_specs=[pl.BlockSpec(memory_space=pl.ANY)] * k + [pl.BlockSpec(memory_space=pltpu.VMEM)] + [pl.BlockSpec(memory_space=pl.ANY)] * 2,
        scratch_shapes=scratch,
        compiler_params=pltpu.CompilerParams(has_side_effects=True, vmem_limit_bytes=LIMIT),
        cost_estimate=pl.CostEstimate(flops=2 * k * TOKENS * ROWS * COLS, bytes_accessed=10**8, transcendentals=0),
        name="gradients",
    )(*lhs, *rhs, gate, up, w_down)[: k + 1]


PART, CHUNK, STRIP = 512, 512, 256
PARTS = COLS // PART
CHUNKS = [pl.ds(r * CHUNK, CHUNK) for r in range(TOKENS // CHUNK)]


def forward_kernel(x_hbm, w_gate, w_up, w_down, gate_out, up_out, act_out, a_hbm, h_hbm, next_hbm, h, a, total, sem):
    j = pl.program_id(0)
    keep_a = pltpu.make_async_copy(a, a_hbm, sem.at[1])

    @pl.when(j == 0)
    def _():
        load = pltpu.make_async_copy(x_hbm, h, sem.at[0])
        load.start()
        load.wait()
        total[...] = jnp.zeros_like(total)

        @pl.loop(0, TOKENS // STRIP)
        def _(block):
            rows = pl.ds(pl.multiple_of(block * STRIP, STRIP), STRIP)
            wide = h[rows, :].astype(jnp.float32)
            a[rows, :] = (wide * scale_of(wide)).astype(jnp.bfloat16)

        keep_a.start()

    for rows in CHUNKS:
        gate, up = f32dot(a[rows, :], w_gate[...]), f32dot(a[rows, :], w_up[...])
        act = (gate * jax.nn.sigmoid(gate) * up).astype(jnp.bfloat16)
        gate_out[rows, :] = gate
        up_out[rows, :] = up
        act_out[rows, :] = act
        total[rows, :] += f32dot(act, w_down[...])

    @pl.when(j == PARTS - 1)
    def _():
        keep_a.wait()

        @pl.loop(0, TOKENS // STRIP)
        def _(block):
            rows = pl.ds(pl.multiple_of(block * STRIP, STRIP), STRIP)
            new = h[rows, :] + total[rows, :].astype(jnp.bfloat16)
            h[rows, :] = new
            wide = new.astype(jnp.float32)
            a[rows, :] = (wide * scale_of(wide)).astype(jnp.bfloat16)

        copies = [pltpu.make_async_copy(h, h_hbm, sem.at[0]), pltpu.make_async_copy(a, next_hbm, sem.at[1])]
        for copy in copies:
            copy.start()
        for copy in copies:
            copy.wait()


def hidden_gradients(gate, up, by_act):
    by_act = by_act.astype(jnp.bfloat16).astype(jnp.float32)
    sig = jax.nn.sigmoid(gate)
    silu = gate * sig
    by_gate = by_act * up * (sig + silu * (1 - sig))
    return (silu * up).astype(jnp.bfloat16), by_gate.astype(jnp.bfloat16), (by_act * silu).astype(jnp.bfloat16)


def top_kernel(
    a_hbm, by_hbm, h_hbm, w_gate, w_up, w_down, act_out, by_gate_out, by_up_out, by_h_hbm, a, by, h, total, sem
):
    j = pl.program_id(0)
    load_h = pltpu.make_async_copy(h_hbm, h, sem.at[2])

    @pl.when(j == 0)
    def _():
        loads = [pltpu.make_async_copy(a_hbm, a, sem.at[0]), pltpu.make_async_copy(by_hbm, by, sem.at[1])]
        for load in loads:
            load.start()
        load_h.start()
        total[...] = jnp.zeros_like(total)
        for load in loads:
            load.wait()

    for rows in CHUNKS:
        gate, up = f32dot(a[rows, :], w_gate[...]), f32dot(a[rows, :], w_up[...])
        act, by_gate, by_up = hidden_gradients(gate, up, f32dot(by[rows, :], w_down[...], 1))
        act_out[rows, :] = act
        by_gate_out[rows, :] = by_gate
        by_up_out[rows, :] = by_up
        total[rows, :] += f32dot(by_gate, w_gate[...], 1) + f32dot(by_up, w_up[...], 1)

    @pl.when(j == PARTS - 1)
    def _():
        load_h.wait()

        @pl.loop(0, TOKENS // STRIP)
        def _(block):
            rows = pl.ds(pl.multiple_of(block * STRIP, STRIP), STRIP)
            by_a = total[rows, :].astype(jnp.bfloat16).astype(jnp.float32)
            wide = h[rows, :].astype(jnp.float32)
            scale = scale_of(wide)
            by_scale = jnp.sum(by_a * wide, -1, keepdims=True)
            by_wide = by_a * scale - wide * (scale * scale * scale * by_scale * (1 / ROWS))
            by[rows, :] = by[rows, :] + by_wide.astype(jnp.bfloat16)

        store = pltpu.make_async_copy(by, by_h_hbm, sem.at[0])
        store.start()
        store.wait()


def wide_part(number):
    return pl.BlockSpec((None, ROWS, PART), lambda j: (number, 0, j))


def tall_part(number):
    return pl.BlockSpec((None, PART, ROWS), lambda j: (number, j, 0))


ANY = pl.BlockSpec(memory_space=pl.ANY)
HIDDEN = pl.BlockSpec((TOKENS, PART), lambda j: (0, j))


def layer_call(kernel, matmuls, in_specs, out_specs, outs, scratch, name):
    return pl.pallas_call(
        kernel,
        grid=(PARTS,),
        out_shape=[jax.ShapeDtypeStruct(shape, dtype) for shape, dtype in outs],
        in_specs=in_specs,
        out_specs=out_specs,
        scratch_shapes=scratch,
        compiler_params=pltpu.CompilerParams(vmem_limit_bytes=LIMIT, dimension_semantics=("arbitrary",)),
        cost_estimate=pl.CostEstimate(flops=2 * matmuls * TOKENS * ROWS * COLS, bytes_accessed=10**8, transcendentals=TOKENS * COLS),
        name=name,
    )


def forward(x, w_gate, w_up, w_down):
    tokens, hidden = (TOKENS, ROWS), (TOKENS, COLS)
    outs = [(hidden, jnp.float32)] * 2 + [(hidden, jnp.bfloat16)] + [(tokens, jnp.bfloat16)] * 3
    scratch = [pltpu.VMEM(tokens, jnp.bfloat16)] * 2 + [pltpu.VMEM(tokens, jnp.float32), pltpu.SemaphoreType.DMA((2,))]
    specs = [ANY, wide_part(0), wide_part(0), tall_part(0)], [HIDDEN] * 3 + [ANY] * 3
    return layer_call(forward_kernel, 3, *specs, outs, scratch, "forward")(x, w_gate, w_up, w_down)


def top(a, by, h, w_gate, w_up, w_down):
    tokens, hidden = (TOKENS, ROWS), (TOKENS, COLS)
    outs = [(hidden, jnp.bfloat16)] * 3 + [(tokens, jnp.bfloat16)]
    scratch = [pltpu.VMEM(tokens, jnp.bfloat16)] * 3 + [pltpu.VMEM(tokens, jnp.float32), pltpu.SemaphoreType.DMA((3,))]
    specs = [ANY] * 3 + [wide_part(1), wide_part(1), tall_part(1)], [HIDDEN] * 3 + [ANY]
    return layer_call(top_kernel, 5, *specs, outs, scratch, "top")(a, by, h, w_gate, w_up, w_down)


def adamw_kernel(turned, factor_ref, g0_ref, g1_ref, w_ref, m_ref, v_ref, w_out, m_out, v_out):
    factor = factor_ref[0, 0]

    rows = w_ref.shape[1]
    strip = 128 if turned else 16

    def update(g_ref):
        @pl.loop(0, rows // strip)
        def _(block):
            at = pl.ds(pl.multiple_of(block * strip, strip), strip)
            g = (g_ref[:, at].astype(jnp.float32).T if turned else g_ref[at, :].astype(jnp.float32)) * factor
            m = 0.9 * m_ref[0, at] + 0.1 * g
            v = 0.95 * v_ref[0, at] + 0.05 * g * g
            w = w_ref[0, at].astype(jnp.float32)
            step = m * lax.rsqrt(v + 1e-8) + 0.1 * w
            w_out[0, at] = (w - 0.02 * step).astype(jnp.bfloat16)
            m_out[0, at] = m
            v_out[0, at] = v

    number = pl.program_id(0)

    @pl.when(number == 0)
    def _():
        update(g0_ref)

    @pl.when(number == 1)
    def _():
        update(g1_ref)


def adamw(factor, g0, g1, w, m, v, rows, turned):
    layers, r, c = w.shape
    blocks = r // rows
    whole = pl.BlockSpec((1, rows, c), lambda number, i: (number, i, 0))
    shape = (c, rows) if turned else (rows, c)
    at = lambda i: (0, i) if turned else (i, 0)
    in0 = pl.BlockSpec(shape, lambda number, i: at(jnp.where(number == 0, i, blocks - 1)))
    in1 = pl.BlockSpec(shape, lambda number, i: at(jnp.where(number == 1, i, 0)))
    return pl.pallas_call(
        functools.partial(adamw_kernel, turned),
        grid=(layers, blocks),
        out_shape=[jax.ShapeDtypeStruct(a.shape, a.dtype) for a in (w, m, v)],
        in_specs=[pl.BlockSpec((1, 1), lambda number, i: (0, 0), memory_space=pltpu.SMEM), in0, in1, whole, whole, whole],
        out_specs=[whole] * 3,
        compiler_params=pltpu.CompilerParams(vmem_limit_bytes=LIMIT, dimension_semantics=("arbitrary", "arbitrary")),
        cost_estimate=pl.CostEstimate(flops=20 * w.size, bytes_accessed=22 * w.size, transcendentals=w.size),
        name="adamw",
    )(factor, g0, g1, w, m, v)


def solution(mesh):
    n = mesh.shape["dp"]

    def step(x, dy, *arrays):
        weights, m, v = (arrays[i : i + 3] for i in (0, 3, 6))
        gate, up, act0, a0, h1, a1 = forward(x[0], *weights)
        act1, by_gate1, by_up1, by_h1 = top(a1, dy[0], h1, *weights)
        lhs, rhs = (dy[0], a1, by_h1, a0), (act1, by_gate1, by_up1, act0)
        down1, gate1, up1, down0, gate0, up0, squares = gradients(lhs, rhs, gate, up, weights[2], (0, 1, 1, 2, 3, 3), n)
        total = jnp.sum(squares)
        factor = jnp.minimum(1.0, 0.5 * lax.rsqrt(total / sum(w.size for w in weights) + 1e-30)).reshape(1, 1)
        pairs = ((gate0, gate1), (up0, up1), (down0, down1))
        new = [
            adamw(factor, *pair, w, m, v, rows, turned)
            for pair, w, m, v, rows, turned in zip(pairs, weights, m, v, (256, 256, 640), (False, False, True), strict=True)
        ]
        return tuple(one[which] for which in range(3) for one in new)

    return jax.shard_map(
        step,
        mesh=mesh,
        in_specs=(P(("rep", "dp"), None, None),) * 2 + (P(None, None, None),) * 9,
        out_specs=(P("rep", None, None),) * 9,
        check_vma=False,
    )
```
